512 devices in a mesh: dp: 2 (over core), layer: 8 (over z), col: 32 (over x, y).
Axes of the slice: x: 4, y: 8, z: 8, core: 2. Of those that a mesh axis runs over, the one named last changes fastest.
Arguments:
- tokens: bfloat16 [16, 256, 1024], P(None, 'dp', 'col'), parts along dimension 1, may hold values from -6 to 6
- w_input: bfloat16 [8, 1024, 4096], P('layer', None, 'col'), may hold values from -0.1875 to 0.1875
- w_recur: bfloat16 [8, 1024, 4096], P('layer', None, 'col'), may hold values from -0.1875 to 0.1875
- bias: float32 [8, 4096], P('layer', 'col'), may hold values from -1 to 5
Outputs:
- top_states: bfloat16 [16, 256, 1024], P('layer', 'dp', 'col'), parts along dimension 1
- final_h: bfloat16 [8, 256, 1024], P('layer', 'dp', 'col'), parts along dimension 1
- final_c: float32 [8, 256, 1024], P('layer', 'dp', 'col'), parts along dimension 1
The draws below stay inside these ranges and needn't reach their ends.
There are 2 independent parts, one for each index of `dp`. The reference program is written for one: setup_inputs(seed, part) draws one part's arguments, and reference() takes and returns one part's arrays. A program takes and returns all parts, laid end to end along the dimension named above; an argument that names none is the same for every part. Nothing has to cross between parts.
All inputs are finite; a program needn't handle non-finite values.
Results may differ from the reference program's by a relative error of at most 0.008.
Values may be sent and summed in bfloat16 or wider, within the bound.
No kernel may reach another device: no remote copies, remote signals or barrier semaphores. Data moves between devices by JAX's collectives and lax.ppermute only.
A program may use at most 64 MiB of HBM per device.

```python
import jax
import jax.numpy as jnp
from jax import lax

H = 1024
GATES = 4096
SENT = 128
TSTEPS = 16
LAYERS = 8


def draw_bias(key, part):
    first, second, third, fourth = jax.random.split(jax.random.fold_in(key, 11), 4)
    others = jax.random.uniform(first, (LAYERS, H, 3), jnp.float32, -1.0, 1.0)
    strong = jax.random.uniform(second, (LAYERS, H), jnp.float32, 3.0, 5.0)
    weak = jax.random.uniform(third, (LAYERS, H), jnp.float32, -1.0, 1.0)
    keeper = jax.random.uniform(fourth, (LAYERS, H)) < 0.5
    forget = jnp.where(keeper, strong, weak)
    stacked = jnp.stack([others[:, :, 0], forget, others[:, :, 1], others[:, :, 2]], axis=-1)
    return stacked.reshape(LAYERS, 4 * H)


def level_of(key, dims, shards, smallest, high):
    factor_of, own = 1.0, jax.random.fold_in(key, 6)
    for position, shards_of in shards:
        steps = jnp.exp(jax.random.uniform(jax.random.fold_in(own, position), (shards_of,), jnp.float32, smallest / len(shards), high / len(shards)))
        factor_of = factor_of * jnp.repeat(steps, dims[position] // shards_of).reshape([-1 if axis == position else 1 for axis in range(len(dims))])
    return factor_of


def gaussian(key, extent, scale, most, cuts=(), dtype=jnp.bfloat16):
    array = jax.random.normal(key, extent, jnp.float32) * scale
    if len(cuts) > 0:
        array = level_of(key, extent, cuts, -0.22, 0.18) * array
    return jnp.clip(array, min=-most, max=most).astype(dtype)


def setup_inputs(seed: int = 0, part: int = 0) -> dict:
    streams_of = jax.random.split(jax.random.key(seed), 5)
    part_splits = jax.random.split(jax.random.fold_in(streams_of[4], part), 5)
    tokens = gaussian(part_splits[0], (TSTEPS, SENT, H), 1.0, 6.0, ((2, 32),))
    w_input = gaussian(streams_of[1], (LAYERS, H, GATES), H ** -0.5, 0.1875, ((0, 8), (2, 32)))
    w_recur = gaussian(streams_of[2], (LAYERS, H, GATES), H ** -0.5, 0.1875, ((0, 8), (2, 32)))
    bias = draw_bias(jax.random.fold_in(streams_of[4], 71), part)
    return {"tokens": tokens, "w_input": w_input, "w_recur": w_recur, "bias": bias}


def run_layer(layer_in, w_in, w_rec, gate_bias):
    sentences = layer_in.shape[1]
    width = w_rec.shape[0]

    def advance(carry, x_step):
        hidden, cell = carry
        gates = jnp.dot(x_step, w_in, preferred_element_type=jnp.float32)
        gates = gates + jnp.dot(hidden, w_rec, preferred_element_type=jnp.float32) + gate_bias
        gates = gates.reshape(sentences, width, 4)
        in_gate = jax.nn.sigmoid(gates[:, :, 0])
        forget = jax.nn.sigmoid(gates[:, :, 1])
        update = jnp.tanh(gates[:, :, 2])
        out_gate = jax.nn.sigmoid(gates[:, :, 3])
        cell = forget * cell + in_gate * update
        hidden = (out_gate * jnp.tanh(cell)).astype(jnp.bfloat16)
        return (hidden, cell), hidden

    start = (jnp.zeros((sentences, width), jnp.bfloat16), jnp.zeros((sentences, width), jnp.float32))
    (hidden, cell), states = lax.scan(advance, start, layer_in)
    return hidden, cell, states


def reference(tokens, w_input, w_recur, bias):
    layer_in = tokens
    last_h = []
    last_c = []
    states = tokens
    for level in range(LAYERS):
        hidden, cell, states = run_layer(layer_in, w_input[level], w_recur[level], bias[level])
        last_h.append(hidden)
        last_c.append(cell)
        if level >= 1:
            layer_in = (states.astype(jnp.float32) + layer_in.astype(jnp.float32)).astype(jnp.bfloat16)
        else:
            layer_in = states
    return states, jnp.stack(last_h), jnp.stack(last_c)
```

```python
import jax
import jax.numpy as jnp
from jax import lax
from jax.experimental import pallas as pl
from jax.experimental.pallas import tpu as pltpu
from jax.sharding import PartitionSpec as P

H = 1024
ROWS = 4
STEPS = 2
LANES = 128
WIDE = 512
BLOCKS = 4 * H // WIDE


def passed_along(block, axis, distance):
    devices = range(lax.axis_size(axis))
    route = [(i - distance, i) for i in devices if i - distance in devices]
    return lax.ppermute(block, axis, route)


def segments_swapped(quad, lane):
    gates = []
    for k in range(4):
        out = None
        for j in range(4):
            shift = (32 * (j - k)) % LANES
            moved = quad[j] if shift == 0 else pltpu.roll(quad[j], shift, 1)
            out = moved if out is None else jnp.where(lane >= 32 * j, moved, out)
        gates.append(out)
    return gates


def stage_kernel(flags, x_got, x_token, h_was, c_was, bias, weights, hs_out, x_out, h_out, c_out, w_in, w_rec, gx, sems):
    active = flags[0] == 1

    @pl.when(active)
    def _():
        copies = []
        for m, target in ((0, w_in), (1, w_rec)):
            for p in range(H // 32):
                copies.append(
                    pltpu.make_async_copy(
                        weights.at[p, m],
                        target.at[:, pl.ds(LANES * p, LANES)],
                        sems.at[m, p],
                    )
                )
        for copy in copies:
            copy.start()
        x = jnp.where(flags[1] == 1, x_token[...].astype(jnp.float32), x_got[...].astype(jnp.float32))
        x_low = x.astype(jnp.bfloat16)
        lane = lax.broadcasted_iota(jnp.int32, (2 * ROWS, LANES), 1)
        row = lax.broadcasted_iota(jnp.int32, (2 * ROWS, H), 0)
        update = (lane >= 64) & (lane < 96)
        scale = jnp.where(update, 1.0, 0.5)
        shift = jnp.where(update, 0.0, 0.5)
        for q in range(BLOCKS):
            for p in range(4):
                copies[4 * q + p].wait()
            part = jnp.dot(x_low, w_in[:, WIDE * q : WIDE * (q + 1)], preferred_element_type=jnp.float32)
            for j in range(4):
                lanes = slice(WIDE * q + LANES * j, WIDE * q + LANES * (j + 1))
                gx[:, lanes] = (part[:, LANES * j : LANES * (j + 1)] + bias[:, lanes]) * scale
        hidden = h_was[...]
        states = []
        for step in range(STEPS):
            h_low = hidden.astype(jnp.bfloat16)
            pieces = []
            for q in range(BLOCKS):
                if step == 0:
                    for p in range(4):
                        copies[H // 32 + 4 * q + p].wait()
                gates = jnp.dot(h_low, w_rec[:, WIDE * q : WIDE * (q + 1)], preferred_element_type=jnp.float32)
                quad = []
                for j in range(4):
                    lanes = slice(WIDE * q + LANES * j, WIDE * q + LANES * (j + 1))
                    z = gates[:, LANES * j : LANES * (j + 1)] * scale + gx[:, lanes]
                    quad.append(jnp.tanh(z) * scale + shift)
                g_in, g_forget, g_update, g_out = segments_swapped(quad, lane)
                here = slice(LANES * q, LANES * (q + 1))
                cell = c_was[:, here] if step == 0 else c_out[:, here]
                cell = g_forget * cell + g_in * g_update
                c_out[:, here] = pltpu.roll(cell, ROWS, 0)
                pieces.append((g_out * jnp.tanh(cell)).astype(jnp.bfloat16).astype(jnp.float32))
            fresh = jnp.concatenate(pieces, axis=1)
            states.append(fresh)
            hidden = pltpu.roll(fresh, ROWS, 0)
        h_out[...] = hidden
        both = jnp.where(row < ROWS, states[0], states[1])
        hs_out[...] = both.astype(jnp.bfloat16)
        x_out[...] = jnp.where(flags[2] == 1, both + x, both).astype(jnp.bfloat16)

    @pl.when(jnp.logical_not(active))
    def _():
        h_out[...] = h_was[...]
        c_out[...] = c_was[...]
        hs_out[...] = x_got[...]
        x_out[...] = x_got[...]


def stage(flags, x_got, x_token, h_was, c_was, bias, weights):
    full = pl.BlockSpec(memory_space=pltpu.VMEM)
    low = jax.ShapeDtypeStruct((2 * ROWS, H), jnp.bfloat16)
    high = jax.ShapeDtypeStruct((2 * ROWS, H), jnp.float32)
    return pl.pallas_call(
        stage_kernel,
        out_shape=(low, low, high, high),
        in_specs=[pl.BlockSpec(memory_space=pltpu.SMEM), full, full, full, full, full, pl.BlockSpec(memory_space=pltpu.HBM)],
        out_specs=(full, full, full, full),
        scratch_shapes=[
            pltpu.VMEM((H, 4 * H), jnp.bfloat16),
            pltpu.VMEM((H, 4 * H), jnp.bfloat16),
            pltpu.VMEM((2 * ROWS, 4 * H), jnp.float32),
            pltpu.SemaphoreType.DMA((2, H // 32)),
        ],
        compiler_params=pltpu.CompilerParams(vmem_limit_bytes=40 * 1024 * 1024),
    )(flags, x_got, x_token, h_was, c_was, bias, weights)


def shards(tokens, w_input, w_recur, bias):
    steps_count, sentences, units = tokens.shape
    layers = lax.axis_size("layer")
    cols = lax.axis_size("col")
    level = lax.axis_index("layer")
    chunks = steps_count // STEPS
    stages = chunks + layers - 1

    at = jnp.arange(4 * units)
    order = (at[:, None] == 4 * (at % units) + at // units).astype(jnp.bfloat16)
    both = jnp.concatenate([w_input[0], w_recur[0]], axis=0)
    both = jnp.dot(both, order, preferred_element_type=jnp.float32).astype(jnp.bfloat16)
    weights = lax.all_gather(both.reshape(2, H, 4 * units), "col")

    local_bias = bias[0].reshape(units, 4).T.reshape(1, 4 * units)
    mine = tokens.reshape(steps_count, cols, ROWS, units).transpose(1, 0, 2, 3).astype(jnp.float32)
    sent = jnp.concatenate([mine.reshape(cols, -1), jnp.broadcast_to(local_bias, (cols, 4 * units))], axis=1)
    got = lax.all_to_all(sent, "col", 0, 0, tiled=True)
    x_first = got[:, : steps_count * ROWS * units].reshape(cols, steps_count * ROWS, units).transpose(1, 0, 2)
    x_first = x_first.reshape(chunks, STEPS * ROWS, H).astype(jnp.bfloat16)
    bias_full = got[:, steps_count * ROWS * units :].reshape(1, 4 * H)

    def section(carry, s):
        x_sent, hidden, cell = carry
        x_got = passed_along(x_sent, "layer", 1)
        chunk = s - level
        active = (chunk >= 0) & (chunk < chunks)
        flags = jnp.stack([active, level == 0, level >= 1]).astype(jnp.int32)
        x_token = lax.dynamic_index_in_dim(x_first, jnp.clip(chunk, 0, chunks - 1), 0, keepdims=False)
        hs, x_next, hidden, cell = stage(flags, x_got, x_token, hidden, cell, bias_full, weights)
        return (x_next, hidden, cell), hs

    zero_x = jnp.zeros((STEPS * ROWS, H), jnp.bfloat16)
    zero_s = jnp.zeros((STEPS * ROWS, H), jnp.float32)
    (_, hidden, cell), states = lax.scan(section, (zero_x, zero_s, zero_s), jnp.arange(stages))

    top = lax.all_to_all(states[layers - 1 :], "layer", 0, 0, tiled=True)[layers - 1]
    rows = jnp.concatenate([top.astype(jnp.float32), hidden[:ROWS], cell[:ROWS]], axis=0)
    sent = rows.reshape(4 * ROWS, cols, units).transpose(1, 0, 2)
    got = lax.all_to_all(sent, "col", 0, 0, tiled=True).reshape(cols, 4, ROWS, units).transpose(1, 0, 2, 3)
    got = got.reshape(4, sentences, units)
    return got[:2].astype(jnp.bfloat16), got[2:3].astype(jnp.bfloat16), got[3:]


def solution(mesh):
    in_specs = (
        P(None, "dp", "col"),
        P("layer", None, "col"),
        P("layer", None, "col"),
        P("layer", "col"),
    )
    out_specs = (P("layer", "dp", "col"), P("layer", "dp", "col"), P("layer", "dp", "col"))
    return jax.shard_map(shards, mesh=mesh, in_specs=in_specs, out_specs=out_specs, check_vma=False)
```

```python
import jax
import jax.numpy as jnp
from jax import lax
from jax.experimental import pallas as pl
from jax.experimental.pallas import tpu as pltpu
from jax.sharding import PartitionSpec as P

H = 1024
ROWS = 4
STEPS = 2
LANES = 128
WIDE = 512
BLOCKS = 4 * H // WIDE


def passed_along(block, axis, distance):
    devices = range(lax.axis_size(axis))
    route = [(i - distance, i) for i in devices if i - distance in devices]
    return lax.ppermute(block, axis, route)


def segments_swapped(quad, lane):
    gates = []
    for k in range(4):
        out = None
        for j in range(4):
            shift = (32 * (j - k)) % LANES
            moved = quad[j] if shift == 0 else pltpu.roll(quad[j], shift, 1)
            out = moved if out is None else jnp.where(lane >= 32 * j, moved, out)
        gates.append(out)
    return gates


def stage_kernel(place, x_got, x_tokens, h_was, c_was, top_was, bias, weights, place_out, x_out, h_out, c_out, top_out, gx, close, sems):
    chunk = place[0]
    level = place[1]
    chunks = x_tokens.shape[0]
    active = (chunk >= 0) & (chunk < chunks)
    place_out[0] = chunk + 1
    place_out[1] = level
    top_out[...] = top_was[...]

    def copy(m, p):
        lanes = pl.ds(LANES * p, LANES)
        return pltpu.make_async_copy(weights.at[p, m], close.at[m, :, lanes], sems.at[m, p])

    def columns(m, q, fresh):
        if fresh:
            for j in range(4):
                copy(m, 4 * q + j).wait()
        return close[m, :, WIDE * q : WIDE * (q + 1)]

    @pl.when(active)
    def _():
        for m in range(2):
            for p in range(H // 32):
                copy(m, p).start()
        x = jnp.where(level == 0, x_tokens[chunk].astype(jnp.float32), x_got[...].astype(jnp.float32))
        x_low = x.astype(jnp.bfloat16)
        lane = lax.broadcasted_iota(jnp.int32, (2 * ROWS, LANES), 1)
        row = lax.broadcasted_iota(jnp.int32, (2 * ROWS, H), 0)
        update = (lane >= 64) & (lane < 96)
        scale = jnp.where(update, 1.0, 0.5)
        shift = jnp.where(update, 0.0, 0.5)
        for q in range(BLOCKS):
            part = jnp.dot(x_low, columns(0, q, True), preferred_element_type=jnp.float32)
            for j in range(4):
                lanes = slice(WIDE * q + LANES * j, WIDE * q + LANES * (j + 1))
                gx[:, lanes] = (part[:, LANES * j : LANES * (j + 1)] + bias[:, lanes]) * scale
        hidden = h_was[...]
        states = []
        for step in range(STEPS):
            h_low = hidden.astype(jnp.bfloat16)
            pieces = []
            for q in range(BLOCKS):
                gates = jnp.dot(h_low, columns(1, q, step == 0), preferred_element_type=jnp.float32)
                quad = []
                for j in range(4):
                    lanes = slice(WIDE * q + LANES * j, WIDE * q + LANES * (j + 1))
                    z = gates[:, LANES * j : LANES * (j + 1)] * scale + gx[:, lanes]
                    quad.append(jnp.tanh(z) * scale + shift)
                g_in, g_forget, g_update, g_out = segments_swapped(quad, lane)
                here = slice(LANES * q, LANES * (q + 1))
                cell = c_was[:, here] if step == 0 else c_out[:, here]
                cell = g_forget * cell + g_in * g_update
                c_out[:, here] = pltpu.roll(cell, ROWS, 0)
                pieces.append((g_out * jnp.tanh(cell)).astype(jnp.bfloat16).astype(jnp.float32))
            fresh = jnp.concatenate(pieces, axis=1)
            states.append(fresh)
            hidden = pltpu.roll(fresh, ROWS, 0)
        h_out[...] = hidden
        both = jnp.where(row < ROWS, states[0], states[1])
        top_out[chunk] = both.astype(jnp.bfloat16)
        x_out[...] = jnp.where(level >= 1, both + x, both).astype(jnp.bfloat16)

    @pl.when(jnp.logical_not(active))
    def _():
        h_out[...] = h_was[...]
        c_out[...] = c_was[...]
        x_out[...] = x_got[...]


def stage(place, x_got, x_tokens, h_was, c_was, top_was, bias, weights):
    full = pl.BlockSpec(memory_space=pltpu.VMEM)
    scalars = pl.BlockSpec(memory_space=pltpu.SMEM)

    def like(x):
        return jax.ShapeDtypeStruct(x.shape, x.dtype)

    return pl.pallas_call(
        stage_kernel,
        out_shape=(like(place), like(x_got), like(h_was), like(c_was), like(top_was)),
        in_specs=[scalars, full, full, full, full, full, full, pl.BlockSpec(memory_space=pltpu.HBM)],
        out_specs=(scalars, full, full, full, full),
        input_output_aliases={0: 0, 3: 2, 4: 3, 5: 4},
        scratch_shapes=[
            pltpu.VMEM((2 * ROWS, 4 * H), jnp.float32),
            pltpu.VMEM((2, H, 4 * H), jnp.bfloat16),
            pltpu.SemaphoreType.DMA((2, H // 32)),
        ],
        compiler_params=pltpu.CompilerParams(vmem_limit_bytes=24 * 1024 * 1024),
    )(place, x_got, x_tokens, h_was, c_was, top_was, bias, weights)


def shards(tokens, w_input, w_recur, bias):
    steps_count, sentences, units = tokens.shape
    layers = lax.axis_size("layer")
    cols = lax.axis_size("col")
    level = lax.axis_index("layer")
    chunks = steps_count // STEPS
    stages = chunks + layers - 1

    at = jnp.arange(4 * units)
    order = (at[:, None] == 4 * (at % units) + at // units).astype(jnp.bfloat16)
    half = jnp.where(lax.axis_index("dp") == 0, w_input[0], w_recur[0])
    half = jnp.dot(half, order, preferred_element_type=jnp.float32).astype(jnp.bfloat16)
    weights = lax.all_gather(half, ("col", "dp")).reshape(cols, 2, H, 4 * units)

    local_bias = bias[0].reshape(units, 4).T.reshape(1, 4 * units)
    mine = tokens.reshape(steps_count, cols, ROWS, units).transpose(1, 0, 2, 3).astype(jnp.float32)
    sent = jnp.concatenate([mine.reshape(cols, -1), jnp.broadcast_to(local_bias, (cols, 4 * units))], axis=1)
    got = lax.all_to_all(sent, "col", 0, 0, tiled=True)
    x_first = got[:, : steps_count * ROWS * units].reshape(cols, steps_count * ROWS, units).transpose(1, 0, 2)
    x_first = x_first.reshape(chunks, STEPS * ROWS, H).astype(jnp.bfloat16)
    bias_full = got[:, steps_count * ROWS * units :].reshape(1, 4 * H)

    def section(_, carry):
        place, x_sent, hidden, cell, top = carry
        x_got = passed_along(x_sent, "layer", 1)
        return tuple(stage(place, x_got, x_first, hidden, cell, top, bias_full, weights))

    place = jnp.stack([-level, level])
    zero_x = jnp.zeros((STEPS * ROWS, H), jnp.bfloat16)
    zero_s = jnp.zeros((STEPS * ROWS, H), jnp.float32)
    zero_t = jnp.zeros((chunks, STEPS * ROWS, H), jnp.bfloat16)
    _, _, hidden, cell, top = lax.fori_loop(0, stages, section, (place, zero_x, zero_s, zero_s, zero_t))

    top = lax.all_to_all(top, "layer", 0, 0, tiled=True)[layers - 1]
    rows = jnp.concatenate([top.astype(jnp.float32), hidden[:ROWS], cell[:ROWS]], axis=0)
    sent = rows.reshape(4 * ROWS, cols, units).transpose(1, 0, 2)
    got = lax.all_to_all(sent, "col", 0, 0, tiled=True).reshape(cols, 4, ROWS, units).transpose(1, 0, 2, 3)
    got = got.reshape(4, sentences, units)
    return got[:2].astype(jnp.bfloat16), got[2:3].astype(jnp.bfloat16), got[3:]


def solution(mesh):
    in_specs = (
        P(None, "dp", "col"),
        P("layer", None, "col"),
        P("layer", None, "col"),
        P("layer", "col"),
    )
    out_specs = (P("layer", "dp", "col"), P("layer", "dp", "col"), P("layer", "dp", "col"))
    return jax.shard_map(shards, mesh=mesh, in_specs=in_specs, out_specs=out_specs, check_vma=False)
```

```python
import jax
import jax.numpy as jnp
from jax import lax
from jax.experimental import pallas as pl
from jax.experimental.pallas import tpu as pltpu
from jax.sharding import PartitionSpec as P

H = 1024
ROWS = 4
STEPS = 2
LANES = 128
WIDE = 512
BLOCKS = 4 * H // WIDE


def passed_along(block, axis, distance):
    devices = range(lax.axis_size(axis))
    route = [(i - distance, i) for i in devices if i - distance in devices]
    return lax.ppermute(block, axis, route)


def segments_swapped(quad, lane):
    gates = []
    for k in range(4):
        out = None
        for j in range(4):
            shift = (32 * (j - k)) % LANES
            moved = quad[j] if shift == 0 else pltpu.roll(quad[j], shift, 1)
            out = moved if out is None else jnp.where(lane >= 32 * j, moved, out)
        gates.append(out)
    return gates


def fetch(weights, close, sems, m, p):
    return pltpu.make_async_copy(weights.at[p, m], close.at[m, :, pl.ds(LANES * p, LANES)], sems.at[m, p])


def columns(weights, close, sems, m, q):
    for j in range(4):
        fetch(weights, close, sems, m, 4 * q + j).wait()
    return close[m, :, WIDE * q : WIDE * (q + 1)]


def early_kernel(h_was, weights, product_out, close, sems):
    for p in range(H // 32):
        fetch(weights, close, sems, 0, p).start()
    h_low = h_was[...].astype(jnp.bfloat16)
    for q in range(BLOCKS):
        part = jnp.dot(h_low, columns(weights, close, sems, 0, q), preferred_element_type=jnp.float32)
        product_out[:, WIDE * q : WIDE * (q + 1)] = part


def late_kernel(place, x_got, x_tokens, product, h_was, c_was, bias, weights, place_out, hs_out, x_out, h_out, c_out, gx, close, sems):
    spot = place[...]
    chunk = jnp.max(spot[0:1, :]).astype(jnp.int32)
    level = jnp.max(spot[4:5, :]).astype(jnp.int32)
    chunks = x_tokens.shape[0]
    active = (chunk >= 0) & (chunk < chunks)
    spot_row = lax.broadcasted_iota(jnp.int32, (2 * ROWS, LANES), 0)
    place_out[...] = jnp.where(spot_row < 4, spot + 1.0, spot)

    @pl.when(active)
    def _():
        for m in (1, 0):
            for p in range(H // 32):
                fetch(weights, close, sems, m, p).start()
        x = jnp.where(level == 0, x_tokens[chunk].astype(jnp.float32), x_got[...].astype(jnp.float32))
        x_low = x.astype(jnp.bfloat16)
        lane = lax.broadcasted_iota(jnp.int32, (2 * ROWS, LANES), 1)
        row = lax.broadcasted_iota(jnp.int32, (2 * ROWS, H), 0)
        update = (lane >= 64) & (lane < 96)
        scale = jnp.where(update, 1.0, 0.5)
        shift = jnp.where(update, 0.0, 0.5)

        def cells(gates, q, cell):
            quad = []
            for j in range(4):
                lanes = slice(WIDE * q + LANES * j, WIDE * q + LANES * (j + 1))
                z = gates[:, LANES * j : LANES * (j + 1)] * scale + gx[:, lanes]
                quad.append(jnp.tanh(z) * scale + shift)
            g_in, g_forget, g_update, g_out = segments_swapped(quad, lane)
            cell = g_forget * cell + g_in * g_update
            c_out[:, LANES * q : LANES * (q + 1)] = pltpu.roll(cell, ROWS, 0)
            return (g_out * jnp.tanh(cell)).astype(jnp.bfloat16).astype(jnp.float32)

        pieces = []
        for q in range(BLOCKS):
            part = jnp.dot(x_low, columns(weights, close, sems, 1, q), preferred_element_type=jnp.float32)
            for j in range(4):
                lanes = slice(WIDE * q + LANES * j, WIDE * q + LANES * (j + 1))
                gx[:, lanes] = (part[:, LANES * j : LANES * (j + 1)] + bias[:, lanes]) * scale
            here = slice(LANES * q, LANES * (q + 1))
            pieces.append(cells(product[:, WIDE * q : WIDE * (q + 1)], q, c_was[:, here]))
        first = jnp.concatenate(pieces, axis=1)
        h_low = pltpu.roll(first, ROWS, 0).astype(jnp.bfloat16)
        pieces = []
        for q in range(BLOCKS):
            part = jnp.dot(h_low, columns(weights, close, sems, 0, q), preferred_element_type=jnp.float32)
            here = slice(LANES * q, LANES * (q + 1))
            pieces.append(cells(part, q, c_out[:, here]))
        second = jnp.concatenate(pieces, axis=1)
        h_out[...] = pltpu.roll(second, ROWS, 0)
        both = jnp.where(row < ROWS, first, second)
        hs_out[...] = both.astype(jnp.bfloat16)
        x_out[...] = jnp.where(level >= 1, both + x, both).astype(jnp.bfloat16)

    @pl.when(jnp.logical_not(active))
    def _():
        h_out[...] = h_was[...]
        c_out[...] = c_was[...]
        hs_out[...] = x_got[...]
        x_out[...] = x_got[...]


FULL = pl.BlockSpec(memory_space=pltpu.VMEM)
FAR = pl.BlockSpec(memory_space=pltpu.HBM)


def early(h_was, weights):
    return pl.pallas_call(
        early_kernel,
        out_shape=jax.ShapeDtypeStruct((2 * ROWS, 4 * H), jnp.float32),
        in_specs=[FULL, FAR],
        out_specs=FULL,
        scratch_shapes=[pltpu.VMEM((1, H, 4 * H), jnp.bfloat16), pltpu.SemaphoreType.DMA((1, H // 32))],
        compiler_params=pltpu.CompilerParams(vmem_limit_bytes=16 * 1024 * 1024),
        cost_estimate=pl.CostEstimate(flops=8_000_000_000, bytes_accessed=8_000_000, transcendentals=0),
    )(h_was, weights)


def late(place, x_got, x_tokens, product, h_was, c_was, bias, weights):
    def like(x):
        return jax.ShapeDtypeStruct(x.shape, x.dtype)

    return pl.pallas_call(
        late_kernel,
        out_shape=(like(place), like(x_got), like(x_got), like(h_was), like(c_was)),
        in_specs=[FULL] * 7 + [FAR],
        out_specs=(FULL,) * 5,
        input_output_aliases={0: 0, 4: 3, 5: 4},
        scratch_shapes=[
            pltpu.VMEM((2 * ROWS, 4 * H), jnp.float32),
            pltpu.VMEM((2, H, 4 * H), jnp.bfloat16),
            pltpu.SemaphoreType.DMA((2, H // 32)),
        ],
        compiler_params=pltpu.CompilerParams(vmem_limit_bytes=24 * 1024 * 1024),
    )(place, x_got, x_tokens, product, h_was, c_was, bias, weights)


def shards(tokens, w_input, w_recur, bias):
    steps_count, sentences, units = tokens.shape
    layers = lax.axis_size("layer")
    cols = lax.axis_size("col")
    level = lax.axis_index("layer")
    chunks = steps_count // STEPS
    stages = chunks + layers - 1

    at = jnp.arange(4 * units)
    order = (at[:, None] == 4 * (at % units) + at // units).astype(jnp.bfloat16)
    half = jnp.where(lax.axis_index("dp") == 0, w_recur[0], w_input[0])
    half = jnp.dot(half, order, preferred_element_type=jnp.float32).astype(jnp.bfloat16)
    weights = lax.all_gather(half, ("col", "dp")).reshape(cols, 2, H, 4 * units)

    local_bias = bias[0].reshape(units, 4).T.reshape(1, 4 * units)
    mine = tokens.reshape(steps_count, cols, ROWS, units).transpose(1, 0, 2, 3).astype(jnp.float32)
    sent = jnp.concatenate([mine.reshape(cols, -1), jnp.broadcast_to(local_bias, (cols, 4 * units))], axis=1)
    got = lax.all_to_all(sent, "col", 0, 0, tiled=True)
    x_first = got[:, : steps_count * ROWS * units].reshape(cols, steps_count * ROWS, units).transpose(1, 0, 2)
    x_first = x_first.reshape(chunks, STEPS * ROWS, H).astype(jnp.bfloat16)
    bias_full = got[:, steps_count * ROWS * units :].reshape(1, 4 * H)

    def section(s, carry):
        place, x_sent, hidden, cell, states = carry
        x_got = passed_along(x_sent, "layer", 1)
        product = early(hidden, weights)
        place, hs, x_next, hidden, cell = late(place, x_got, x_first, product, hidden, cell, bias_full, weights)
        states = lax.dynamic_update_index_in_dim(states, hs, s, 0)
        return place, x_next, hidden, cell, states

    row = jnp.arange(2 * ROWS)[:, None]
    place = jnp.where(row < 4, -level, level) * jnp.ones((1, LANES), jnp.float32)
    zero_x = jnp.zeros((STEPS * ROWS, H), jnp.bfloat16)
    zero_s = jnp.zeros((STEPS * ROWS, H), jnp.float32)
    zero_t = jnp.zeros((stages, STEPS * ROWS, H), jnp.bfloat16)
    _, _, hidden, cell, states = lax.fori_loop(0, stages, section, (place, zero_x, zero_s, zero_s, zero_t))

    top = lax.all_to_all(states[layers - 1 :], "layer", 0, 0, tiled=True)[layers - 1]
    rows = jnp.concatenate([top.astype(jnp.float32), hidden[:ROWS], cell[:ROWS]], axis=0)
    sent = rows.reshape(4 * ROWS, cols, units).transpose(1, 0, 2)
    got = lax.all_to_all(sent, "col", 0, 0, tiled=True).reshape(cols, 4, ROWS, units).transpose(1, 0, 2, 3)
    got = got.reshape(4, sentences, units)
    return got[:2].astype(jnp.bfloat16), got[2:3].astype(jnp.bfloat16), got[3:]


def solution(mesh):
    in_specs = (
        P(None, "dp", "col"),
        P("layer", None, "col"),
        P("layer", None, "col"),
        P("layer", "col"),
    )
    out_specs = (P("layer", "dp", "col"), P("layer", "dp", "col"), P("layer", "dp", "col"))
    return jax.shard_map(shards, mesh=mesh, in_specs=in_specs, out_specs=out_specs, check_vma=False)
```

```python
import jax
import jax.numpy as jnp
from jax import lax
from jax.experimental import pallas as pl
from jax.experimental.pallas import tpu as pltpu
from jax.sharding import PartitionSpec as P

H = 1024
ROWS = 4
STEPS = 2
LANES = 128
WIDE = 512
BLOCKS = 4 * H // WIDE
KEPT = 2


def passed_along(block, axis, distance):
    devices = range(lax.axis_size(axis))
    route = [(i - distance, i) for i in devices if i - distance in devices]
    return lax.ppermute(block, axis, route)


def segments_swapped(quad, lane):
    gates = []
    for k in range(4):
        out = None
        for j in range(4):
            shift = (32 * (j - k)) % LANES
            moved = quad[j] if shift == 0 else pltpu.roll(quad[j], shift, 1)
            out = moved if out is None else jnp.where(lane >= 32 * j, moved, out)
        gates.append(out)
    return gates


def fetch(weights, close, sems, m, p):
    return pltpu.make_async_copy(weights.at[p, m], close.at[m, :, pl.ds(LANES * p, LANES)], sems.at[m, p])


def columns(weights, close, sems, m, q):
    for j in range(4):
        fetch(weights, close, sems, m, 4 * q + j).wait()
    return close[m, :, WIDE * q : WIDE * (q + 1)]


def keep_kernel(weights, kept, sems):
    copies = [
        pltpu.make_async_copy(weights.at[p, 1], kept.at[:, pl.ds(LANES * p, LANES)], sems.at[p]) for p in range(4 * KEPT)
    ]
    for copy in copies:
        copy.start()
    for copy in copies:
        copy.wait()


def early_kernel(h_was, weights, product_out, close, sems):
    for p in range(H // 32):
        fetch(weights, close, sems, 0, p).start()
    h_low = h_was[...].astype(jnp.bfloat16)
    for q in range(BLOCKS):
        part = jnp.dot(h_low, columns(weights, close, sems, 0, q), preferred_element_type=jnp.float32)
        product_out[:, WIDE * q : WIDE * (q + 1)] = part


def late_kernel(place, x_got, x_tokens, product, h_was, c_was, bias, kept, weights, place_out, hs_out, x_out, h_out, c_out, gx, close, sems):
    spot = place[...]
    chunk = jnp.max(spot[0:1, :]).astype(jnp.int32)
    level = jnp.max(spot[4:5, :]).astype(jnp.int32)
    chunks = x_tokens.shape[0]
    active = (chunk >= 0) & (chunk < chunks)
    spot_row = lax.broadcasted_iota(jnp.int32, (2 * ROWS, LANES), 0)
    place_out[...] = jnp.where(spot_row < 4, spot + 1.0, spot)

    @pl.when(active)
    def _():
        for m, done in ((1, 4 * KEPT), (0, 0)):
            for p in range(done, H // 32):
                fetch(weights, close, sems, m, p).start()
        x = jnp.where(level == 0, x_tokens[chunk].astype(jnp.float32), x_got[...].astype(jnp.float32))
        x_low = x.astype(jnp.bfloat16)
        lane = lax.broadcasted_iota(jnp.int32, (2 * ROWS, LANES), 1)
        row = lax.broadcasted_iota(jnp.int32, (2 * ROWS, H), 0)
        update = (lane >= 64) & (lane < 96)
        scale = jnp.where(update, 1.0, 0.5)
        shift = jnp.where(update, 0.0, 0.5)

        def cells(gates, q, cell):
            quad = []
            for j in range(4):
                lanes = slice(WIDE * q + LANES * j, WIDE * q + LANES * (j + 1))
                z = gates[:, LANES * j : LANES * (j + 1)] * scale + gx[:, lanes]
                quad.append(jnp.tanh(z) * scale + shift)
            g_in, g_forget, g_update, g_out = segments_swapped(quad, lane)
            cell = g_forget * cell + g_in * g_update
            c_out[:, LANES * q : LANES * (q + 1)] = pltpu.roll(cell, ROWS, 0)
            return (g_out * jnp.tanh(cell)).astype(jnp.bfloat16).astype(jnp.float32)

        pieces = []
        for q in range(BLOCKS):
            if q < KEPT:
                block = kept[:, WIDE * q : WIDE * (q + 1)]
            else:
                block = columns(weights, close, sems, 1, q)
            part = jnp.dot(x_low, block, preferred_element_type=jnp.float32)
            for j in range(4):
                lanes = slice(WIDE * q + LANES * j, WIDE * q + LANES * (j + 1))
                gx[:, lanes] = (part[:, LANES * j : LANES * (j + 1)] + bias[:, lanes]) * scale
            here = slice(LANES * q, LANES * (q + 1))
            pieces.append(cells(product[:, WIDE * q : WIDE * (q + 1)], q, c_was[:, here]))
        first = jnp.concatenate(pieces, axis=1)
        h_low = pltpu.roll(first, ROWS, 0).astype(jnp.bfloat16)
        pieces = []
        for q in range(BLOCKS):
            part = jnp.dot(h_low, columns(weights, close, sems, 0, q), preferred_element_type=jnp.float32)
            here = slice(LANES * q, LANES * (q + 1))
            pieces.append(cells(part, q, c_out[:, here]))
        second = jnp.concatenate(pieces, axis=1)
        h_out[...] = pltpu.roll(second, ROWS, 0)
        both = jnp.where(row < ROWS, first, second)
        hs_out[...] = both.astype(jnp.bfloat16)
        x_out[...] = jnp.where(level >= 1, both + x, both).astype(jnp.bfloat16)

    @pl.when(jnp.logical_not(active))
    def _():
        h_out[...] = h_was[...]
        c_out[...] = c_was[...]
        hs_out[...] = x_got[...]
        x_out[...] = x_got[...]


FULL = pl.BlockSpec(memory_space=pltpu.VMEM)
FAR = pl.BlockSpec(memory_space=pltpu.HBM)


def early(h_was, weights):
    return pl.pallas_call(
        early_kernel,
        out_shape=jax.ShapeDtypeStruct((2 * ROWS, 4 * H), jnp.float32),
        in_specs=[FULL, FAR],
        out_specs=FULL,
        scratch_shapes=[pltpu.VMEM((1, H, 4 * H), jnp.bfloat16), pltpu.SemaphoreType.DMA((1, H // 32))],
        compiler_params=pltpu.CompilerParams(vmem_limit_bytes=16 * 1024 * 1024),
        cost_estimate=pl.CostEstimate(flops=8_000_000_000, bytes_accessed=8_000_000, transcendentals=0),
    )(h_was, weights)


def keep(weights):
    return pl.pallas_call(
        keep_kernel,
        out_shape=jax.ShapeDtypeStruct((H, WIDE * KEPT), jnp.bfloat16),
        in_specs=[FAR],
        out_specs=FULL,
        scratch_shapes=[pltpu.SemaphoreType.DMA((4 * KEPT,))],
        compiler_params=pltpu.CompilerParams(vmem_limit_bytes=16 * 1024 * 1024),
    )(weights)


def late(place, x_got, x_tokens, product, h_was, c_was, bias, kept, weights):
    def like(x):
        return jax.ShapeDtypeStruct(x.shape, x.dtype)

    return pl.pallas_call(
        late_kernel,
        out_shape=(like(place), like(x_got), like(x_got), like(h_was), like(c_was)),
        in_specs=[FULL] * 8 + [FAR],
        out_specs=(FULL,) * 5,
        input_output_aliases={0: 0, 4: 3, 5: 4},
        scratch_shapes=[
            pltpu.VMEM((2 * ROWS, 4 * H), jnp.float32),
            pltpu.VMEM((2, H, 4 * H), jnp.bfloat16),
            pltpu.SemaphoreType.DMA((2, H // 32)),
        ],
        compiler_params=pltpu.CompilerParams(vmem_limit_bytes=24 * 1024 * 1024),
    )(place, x_got, x_tokens, product, h_was, c_was, bias, kept, weights)


def shards(tokens, w_input, w_recur, bias):
    steps_count, sentences, units = tokens.shape
    layers = lax.axis_size("layer")
    cols = lax.axis_size("col")
    level = lax.axis_index("layer")
    chunks = steps_count // STEPS
    stages = chunks + layers - 1

    at = jnp.arange(4 * units)
    order = (at[:, None] == 4 * (at % units) + at // units).astype(jnp.bfloat16)
    half = jnp.where(lax.axis_index("dp") == 0, w_recur[0], w_input[0])
    half = jnp.dot(half, order, preferred_element_type=jnp.float32).astype(jnp.bfloat16)
    weights = lax.all_gather(half, ("col", "dp")).reshape(cols, 2, H, 4 * units)

    kept = keep(weights)

    local_bias = bias[0].reshape(units, 4).T.reshape(1, 4 * units)
    mine = tokens.reshape(steps_count, cols, ROWS, units).transpose(1, 0, 2, 3).astype(jnp.float32)
    sent = jnp.concatenate([mine.reshape(cols, -1), jnp.broadcast_to(local_bias, (cols, 4 * units))], axis=1)
    got = lax.all_to_all(sent, "col", 0, 0, tiled=True)
    x_first = got[:, : steps_count * ROWS * units].reshape(cols, steps_count * ROWS, units).transpose(1, 0, 2)
    x_first = x_first.reshape(chunks, STEPS * ROWS, H).astype(jnp.bfloat16)
    bias_full = got[:, steps_count * ROWS * units :].reshape(1, 4 * H)

    def section(s, carry):
        place, x_sent, hidden, cell, states = carry
        x_got = passed_along(x_sent, "layer", 1)
        product = early(hidden, weights)
        place, hs, x_next, hidden, cell = late(
            place, x_got, x_first, product, hidden, cell, bias_full, kept, weights
        )
        states = lax.dynamic_update_index_in_dim(states, hs, s, 0)
        return place, x_next, hidden, cell, states

    row = jnp.arange(2 * ROWS)[:, None]
    place = jnp.where(row < 4, -level, level) * jnp.ones((1, LANES), jnp.float32)
    zero_x = jnp.zeros((STEPS * ROWS, H), jnp.bfloat16)
    zero_s = jnp.zeros((STEPS * ROWS, H), jnp.float32)
    zero_t = jnp.zeros((stages, STEPS * ROWS, H), jnp.bfloat16)
    _, _, hidden, cell, states = lax.fori_loop(0, stages, section, (place, zero_x, zero_s, zero_s, zero_t))

    top = lax.all_to_all(states[layers - 1 :], "layer", 0, 0, tiled=True)[layers - 1]
    rows = jnp.concatenate([top.astype(jnp.float32), hidden[:ROWS], cell[:ROWS]], axis=0)
    sent = rows.reshape(4 * ROWS, cols, units).transpose(1, 0, 2)
    got = lax.all_to_all(sent, "col", 0, 0, tiled=True).reshape(cols, 4, ROWS, units).transpose(1, 0, 2, 3)
    got = got.reshape(4, sentences, units)
    return got[:2].astype(jnp.bfloat16), got[2:3].astype(jnp.bfloat16), got[3:]


def solution(mesh):
    in_specs = (
        P(None, "dp", "col"),
        P("layer", None, "col"),
        P("layer", None, "col"),
        P("layer", "col"),
    )
    out_specs = (P("layer", "dp", "col"), P("layer", "dp", "col"), P("layer", "dp", "col"))
    return jax.shard_map(shards, mesh=mesh, in_specs=in_specs, out_specs=out_specs, check_vma=False)
```

```python
import jax
import jax.numpy as jnp
from jax import lax
from jax.experimental import pallas as pl
from jax.experimental.pallas import tpu as pltpu
from jax.sharding import PartitionSpec as P

H = 1024
ROWS = 4
STEPS = 2
LANES = 128
WIDE = 512
BLOCKS = 4 * H // WIDE
KEPT = 2


def passed_along(block, axis, distance):
    devices = range(lax.axis_size(axis))
    route = [(i - distance, i) for i in devices if i - distance in devices]
    return lax.ppermute(block, axis, route)


def segments_swapped(quad, lane):
    gates = []
    for k in range(4):
        out = None
        for j in range(4):
            shift = (32 * (j - k)) % LANES
            moved = quad[j] if shift == 0 else pltpu.roll(quad[j], shift, 1)
            out = moved if out is None else jnp.where(lane >= 32 * j, moved, out)
        gates.append(out)
    return gates


def fetch(weights, close, sems, m, p):
    return pltpu.make_async_copy(weights.at[p, m], close.at[m, :, pl.ds(LANES * p, LANES)], sems.at[m, p])


def columns(weights, close, sems, m, q):
    for j in range(4):
        fetch(weights, close, sems, m, 4 * q + j).wait()
    return close[m, :, WIDE * q : WIDE * (q + 1)]


def keep_kernel(weights, kept, sems):
    copies = [
        pltpu.make_async_copy(weights.at[p, 1], kept.at[:, pl.ds(LANES * p, LANES)], sems.at[p]) for p in range(4 * KEPT)
    ]
    for copy in copies:
        copy.start()
    for copy in copies:
        copy.wait()


def early_kernel(h_was, weights, product_out, close, sems):
    for p in range(H // 32):
        fetch(weights, close, sems, 0, p).start()
    h_low = h_was[...].astype(jnp.bfloat16)
    for q in range(BLOCKS):
        part = jnp.dot(h_low, columns(weights, close, sems, 0, q), preferred_element_type=jnp.float32)
        product_out[:, WIDE * q : WIDE * (q + 1)] = part


def late_kernel(place, x_got, x_tokens, product, h_was, c_was, bias, kept, weights, place_out, hs_out, x_out, h_out, c_out, gx, close, sems):
    spot = place[...]
    chunk = jnp.max(spot[0:1, :]).astype(jnp.int32)
    level = jnp.max(spot[4:5, :]).astype(jnp.int32)
    chunks = x_tokens.shape[0]
    active = (chunk >= 0) & (chunk < chunks)
    spot_row = lax.broadcasted_iota(jnp.int32, (2 * ROWS, LANES), 0)
    place_out[...] = jnp.where(spot_row < 4, spot + 1.0, spot)

    @pl.when(active)
    def _():
        for m, done in ((1, 4 * KEPT), (0, 0)):
            for p in range(done, H // 32):
                fetch(weights, close, sems, m, p).start()
        x = jnp.where(level == 0, x_tokens[chunk].astype(jnp.float32), x_got[...].astype(jnp.float32))
        x_low = x.astype(jnp.bfloat16)
        lane = lax.broadcasted_iota(jnp.int32, (2 * ROWS, LANES), 1)
        row = lax.broadcasted_iota(jnp.int32, (2 * ROWS, H), 0)
        update = (lane >= 64) & (lane < 96)
        scale = jnp.where(update, 1.0, 0.5)
        shift = jnp.where(update, 0.0, 0.5)

        def cells(gates, q, cell):
            quad = []
            for j in range(4):
                lanes = slice(WIDE * q + LANES * j, WIDE * q + LANES * (j + 1))
                z = gates[:, LANES * j : LANES * (j + 1)] * scale + gx[:, lanes]
                quad.append(jnp.tanh(z) * scale + shift)
            g_in, g_forget, g_update, g_out = segments_swapped(quad, lane)
            cell = g_forget * cell + g_in * g_update
            c_out[:, LANES * q : LANES * (q + 1)] = pltpu.roll(cell, ROWS, 0)
            return (g_out * jnp.tanh(cell)).astype(jnp.bfloat16).astype(jnp.float32)

        pieces = []
        for q in range(BLOCKS):
            if q < KEPT:
                block = kept[:, WIDE * q : WIDE * (q + 1)]
            else:
                block = columns(weights, close, sems, 1, q)
            part = jnp.dot(x_low, block, preferred_element_type=jnp.float32)
            for j in range(4):
                lanes = slice(WIDE * q + LANES * j, WIDE * q + LANES * (j + 1))
                gx[:, lanes] = (part[:, LANES * j : LANES * (j + 1)] + bias[:, lanes]) * scale
            here = slice(LANES * q, LANES * (q + 1))
            pieces.append(cells(product[:, WIDE * q : WIDE * (q + 1)], q, c_was[:, here]))
        first = jnp.concatenate(pieces, axis=1)
        h_low = pltpu.roll(first, ROWS, 0).astype(jnp.bfloat16)
        pieces = []
        for q in range(BLOCKS):
            part = jnp.dot(h_low, columns(weights, close, sems, 0, q), preferred_element_type=jnp.float32)
            here = slice(LANES * q, LANES * (q + 1))
            pieces.append(cells(part, q, c_out[:, here]))
        second = jnp.concatenate(pieces, axis=1)
        h_out[...] = pltpu.roll(second, ROWS, 0)
        both = jnp.where(row < ROWS, first, second)
        hs_out[...] = both.astype(jnp.bfloat16)
        x_out[...] = jnp.where(level >= 1, both + x, both).astype(jnp.bfloat16)

    @pl.when(jnp.logical_not(active))
    def _():
        h_out[...] = h_was[...]
        c_out[...] = c_was[...]
        hs_out[...] = x_got[...]
        x_out[...] = x_got[...]


FULL = pl.BlockSpec(memory_space=pltpu.VMEM)
FAR = pl.BlockSpec(memory_space=pltpu.HBM)


def early(h_was, weights):
    return pl.pallas_call(
        early_kernel,
        out_shape=jax.ShapeDtypeStruct((2 * ROWS, 4 * H), jnp.float32),
        in_specs=[FULL, FAR],
        out_specs=FULL,
        scratch_shapes=[pltpu.VMEM((1, H, 4 * H), jnp.bfloat16), pltpu.SemaphoreType.DMA((1, H // 32))],
        compiler_params=pltpu.CompilerParams(vmem_limit_bytes=16 * 1024 * 1024),
        cost_estimate=pl.CostEstimate(flops=8_000_000_000, bytes_accessed=8_000_000, transcendentals=0),
    )(h_was, weights)


def keep(weights):
    return pl.pallas_call(
        keep_kernel,
        out_shape=jax.ShapeDtypeStruct((H, WIDE * KEPT), jnp.bfloat16),
        in_specs=[FAR],
        out_specs=FULL,
        scratch_shapes=[pltpu.SemaphoreType.DMA((4 * KEPT,))],
        compiler_params=pltpu.CompilerParams(vmem_limit_bytes=16 * 1024 * 1024),
    )(weights)


def late(place, x_got, x_tokens, product, h_was, c_was, bias, kept, weights):
    def like(x):
        return jax.ShapeDtypeStruct(x.shape, x.dtype)

    return pl.pallas_call(
        late_kernel,
        out_shape=(like(place), like(x_got), like(x_got), like(h_was), like(c_was)),
        in_specs=[FULL] * 8 + [FAR],
        out_specs=(FULL,) * 5,
        input_output_aliases={0: 0, 4: 3, 5: 4},
        scratch_shapes=[
            pltpu.VMEM((2 * ROWS, 4 * H), jnp.float32),
            pltpu.VMEM((2, H, 4 * H), jnp.bfloat16),
            pltpu.SemaphoreType.DMA((2, H // 32)),
        ],
        compiler_params=pltpu.CompilerParams(vmem_limit_bytes=24 * 1024 * 1024),
    )(place, x_got, x_tokens, product, h_was, c_was, bias, kept, weights)


def shards(tokens, w_input, w_recur, bias):
    steps_count, sentences, units = tokens.shape
    layers = lax.axis_size("layer")
    cols = lax.axis_size("col")
    level = lax.axis_index("layer")
    chunks = steps_count // STEPS
    stages = chunks + layers - 1

    at = jnp.arange(4 * units)
    order = (at[:, None] == 4 * (at % units) + at // units).astype(jnp.bfloat16)
    half = jnp.where(lax.axis_index("dp") == 0, w_recur[0], w_input[0])
    half = jnp.dot(half, order, preferred_element_type=jnp.float32).astype(jnp.bfloat16)
    weights = lax.all_gather(half, ("col", "dp")).reshape(cols, 2, H, 4 * units)

    kept = keep(weights)

    local_bias = bias[0].reshape(units, 4).T.reshape(1, 4 * units)
    mine = tokens.reshape(steps_count, cols, ROWS, units).transpose(1, 0, 2, 3).astype(jnp.float32)
    sent = jnp.concatenate([mine.reshape(cols, -1), jnp.broadcast_to(local_bias, (cols, 4 * units))], axis=1)
    got = lax.all_to_all(sent, "col", 0, 0, tiled=True)
    x_first = got[:, : steps_count * ROWS * units].reshape(cols, steps_count * ROWS, units).transpose(1, 0, 2)
    x_first = x_first.reshape(chunks, STEPS * ROWS, H).astype(jnp.bfloat16)
    bias_full = got[:, steps_count * ROWS * units :].reshape(1, 4 * H)

    def section(s, carry):
        place, x_sent, hidden, cell, states = carry
        x_got = passed_along(x_sent, "layer", 1)
        product = early(hidden, weights)
        place, hs, x_next, hidden, cell = late(
            place, x_got, x_first, product, hidden, cell, bias_full, kept, weights
        )
        states = lax.dynamic_update_index_in_dim(states, hs, jnp.maximum(s - (layers - 2), 0), 0)
        return place, x_next, hidden, cell, states

    row = jnp.arange(2 * ROWS)[:, None]
    place = jnp.where(row < 4, -level, level) * jnp.ones((1, LANES), jnp.float32)
    zero_x = jnp.zeros((STEPS * ROWS, H), jnp.bfloat16)
    zero_s = jnp.zeros((STEPS * ROWS, H), jnp.float32)
    zero_t = jnp.zeros((chunks + 1, STEPS * ROWS, H), jnp.bfloat16)
    carry = lax.fori_loop(0, stages - 1, section, (place, zero_x, zero_s, zero_s, zero_t))

    moved = lax.all_to_all(carry[4][1:], "layer", 0, 0, tiled=True)[layers - 1]
    _, _, hidden, cell, states = section(stages - 1, carry)
    top = jnp.where(level == layers - 1, states[chunks], moved)
    rows = jnp.concatenate([top.astype(jnp.float32), hidden[:ROWS], cell[:ROWS]], axis=0)
    sent = rows.reshape(4 * ROWS, cols, units).transpose(1, 0, 2)
    got = lax.all_to_all(sent, "col", 0, 0, tiled=True).reshape(cols, 4, ROWS, units).transpose(1, 0, 2, 3)
    got = got.reshape(4, sentences, units)
    return got[:2].astype(jnp.bfloat16), got[2:3].astype(jnp.bfloat16), got[3:]


def solution(mesh):
    in_specs = (
        P(None, "dp", "col"),
        P("layer", None, "col"),
        P("layer", None, "col"),
        P("layer", "col"),
    )
    out_specs = (P("layer", "dp", "col"), P("layer", "dp", "col"), P("layer", "dp", "col"))
    return jax.shard_map(shards, mesh=mesh, in_specs=in_specs, out_specs=out_specs, check_vma=False)
```

```python
import jax
import jax.numpy as jnp
from jax import lax
from jax.experimental import pallas as pl
from jax.experimental.pallas import tpu as pltpu
from jax.sharding import PartitionSpec as P

H = 1024
ROWS = 4
STEPS = 2
LANES = 128
WIDE = 512
BLOCKS = 4 * H // WIDE
KEPT = 2


def passed_along(block, axis, distance):
    devices = range(lax.axis_size(axis))
    route = [(i - distance, i) for i in devices if i - distance in devices]
    return lax.ppermute(block, axis, route)


def segments_swapped(quad, lane):
    gates = []
    for k in range(4):
        out = None
        for j in range(4):
            shift = (32 * (j - k)) % LANES
            moved = quad[j] if shift == 0 else pltpu.roll(quad[j], shift, 1)
            out = moved if out is None else jnp.where(lane >= 32 * j, moved, out)
        gates.append(out)
    return gates


def fetch(weights, close, sems, m, p):
    return pltpu.make_async_copy(weights.at[p, m], close.at[m, :, pl.ds(LANES * p, LANES)], sems.at[m, p])


def columns(weights, close, sems, m, q):
    for j in range(4):
        fetch(weights, close, sems, m, 4 * q + j).wait()
    return close[m, :, WIDE * q : WIDE * (q + 1)]


def keep_kernel(weights, kept, sems):
    copies = [
        pltpu.make_async_copy(weights.at[p, 1], kept.at[:, pl.ds(LANES * p, LANES)], sems.at[p]) for p in range(4 * KEPT)
    ]
    for copy in copies:
        copy.start()
    for copy in copies:
        copy.wait()


def early_kernel(h_was, weights, product_out, close, sems):
    for p in range(H // 32):
        fetch(weights, close, sems, 0, p).start()
    h_low = h_was[...].astype(jnp.bfloat16)
    for q in range(BLOCKS):
        part = jnp.dot(h_low, columns(weights, close, sems, 0, q), preferred_element_type=jnp.float32)
        product_out[:, WIDE * q : WIDE * (q + 1)] = part


def late_kernel(place, x_got, x_tokens, product, h_was, c_was, bias, kept, weights, place_out, hs_out, x_out, h_out, c_out, gx, close, sems):
    spot = place[...]
    chunk = jnp.max(spot[0:1, :]).astype(jnp.int32)
    level = jnp.max(spot[4:5, :]).astype(jnp.int32)
    chunks = x_tokens.shape[0]
    active = (chunk >= 0) & (chunk < chunks)
    spot_row = lax.broadcasted_iota(jnp.int32, (2 * ROWS, LANES), 0)
    place_out[...] = jnp.where(spot_row < 4, spot + 1.0, spot)

    @pl.when(active)
    def _():
        for m, done in ((1, 4 * KEPT), (0, 0)):
            for p in range(done, H // 32):
                fetch(weights, close, sems, m, p).start()
        x = jnp.where(level == 0, x_tokens[chunk].astype(jnp.float32), x_got[...].astype(jnp.float32))
        x_low = x.astype(jnp.bfloat16)
        lane = lax.broadcasted_iota(jnp.int32, (2 * ROWS, LANES), 1)
        row = lax.broadcasted_iota(jnp.int32, (2 * ROWS, H), 0)
        update = (lane >= 64) & (lane < 96)
        scale = jnp.where(update, 1.0, 0.5)
        shift = jnp.where(update, 0.0, 0.5)

        def cells(gates, q, cell):
            quad = []
            for j in range(4):
                lanes = slice(WIDE * q + LANES * j, WIDE * q + LANES * (j + 1))
                z = gates[:, LANES * j : LANES * (j + 1)] * scale + gx[:, lanes]
                quad.append(jnp.tanh(z) * scale + shift)
            g_in, g_forget, g_update, g_out = segments_swapped(quad, lane)
            cell = g_forget * cell + g_in * g_update
            c_out[:, LANES * q : LANES * (q + 1)] = pltpu.roll(cell, ROWS, 0)
            return (g_out * jnp.tanh(cell)).astype(jnp.bfloat16).astype(jnp.float32)

        pieces = []
        for q in range(BLOCKS):
            if q < KEPT:
                block = kept[:, WIDE * q : WIDE * (q + 1)]
            else:
                block = columns(weights, close, sems, 1, q)
            part = jnp.dot(x_low, block, preferred_element_type=jnp.float32)
            for j in range(4):
                lanes = slice(WIDE * q + LANES * j, WIDE * q + LANES * (j + 1))
                gx[:, lanes] = (part[:, LANES * j : LANES * (j + 1)] + bias[:, lanes]) * scale
            here = slice(LANES * q, LANES * (q + 1))
            pieces.append(cells(product[:, WIDE * q : WIDE * (q + 1)], q, c_was[:, here]))
        first = jnp.concatenate(pieces, axis=1)
        h_low = pltpu.roll(first, ROWS, 0).astype(jnp.bfloat16)
        pieces = []
        for q in range(BLOCKS):
            part = jnp.dot(h_low, columns(weights, close, sems, 0, q), preferred_element_type=jnp.float32)
            here = slice(LANES * q, LANES * (q + 1))
            pieces.append(cells(part, q, c_out[:, here]))
        second = jnp.concatenate(pieces, axis=1)
        h_out[...] = pltpu.roll(second, ROWS, 0)
        both = jnp.where(row < ROWS, first, second)
        hs_out[...] = both.astype(jnp.bfloat16)
        x_out[...] = jnp.where(level >= 1, both + x, both).astype(jnp.bfloat16)

    @pl.when(jnp.logical_not(active))
    def _():
        h_out[...] = h_was[...]
        c_out[...] = c_was[...]
        hs_out[...] = x_got[...]
        x_out[...] = x_got[...]


FULL = pl.BlockSpec(memory_space=pltpu.VMEM)
FAR = pl.BlockSpec(memory_space=pltpu.HBM)


def early(h_was, weights):
    return pl.pallas_call(
        early_kernel,
        out_shape=jax.ShapeDtypeStruct((2 * ROWS, 4 * H), jnp.float32),
        in_specs=[FULL, FAR],
        out_specs=FULL,
        scratch_shapes=[pltpu.VMEM((1, H, 4 * H), jnp.bfloat16), pltpu.SemaphoreType.DMA((1, H // 32))],
        compiler_params=pltpu.CompilerParams(vmem_limit_bytes=16 * 1024 * 1024),
        cost_estimate=pl.CostEstimate(flops=8_000_000_000, bytes_accessed=8_000_000, transcendentals=0),
    )(h_was, weights)


def keep(weights):
    return pl.pallas_call(
        keep_kernel,
        out_shape=jax.ShapeDtypeStruct((H, WIDE * KEPT), jnp.bfloat16),
        in_specs=[FAR],
        out_specs=FULL,
        scratch_shapes=[pltpu.SemaphoreType.DMA((4 * KEPT,))],
        compiler_params=pltpu.CompilerParams(vmem_limit_bytes=16 * 1024 * 1024),
    )(weights)


def late(place, x_got, x_tokens, product, h_was, c_was, bias, kept, weights):
    def like(x):
        return jax.ShapeDtypeStruct(x.shape, x.dtype)

    return pl.pallas_call(
        late_kernel,
        out_shape=(like(place), like(x_got), like(x_got), like(h_was), like(c_was)),
        in_specs=[FULL] * 8 + [FAR],
        out_specs=(FULL,) * 5,
        input_output_aliases={0: 0, 4: 3, 5: 4},
        scratch_shapes=[
            pltpu.VMEM((2 * ROWS, 4 * H), jnp.float32),
            pltpu.VMEM((2, H, 4 * H), jnp.bfloat16),
            pltpu.SemaphoreType.DMA((2, H // 32)),
        ],
        compiler_params=pltpu.CompilerParams(vmem_limit_bytes=24 * 1024 * 1024),
    )(place, x_got, x_tokens, product, h_was, c_was, bias, kept, weights)


def shards(tokens, w_input, w_recur, bias):
    steps_count, sentences, units = tokens.shape
    layers = lax.axis_size("layer")
    cols = lax.axis_size("col")
    level = lax.axis_index("layer")
    chunks = steps_count // STEPS
    stages = chunks + layers - 1

    at = jnp.arange(4 * units)
    order = (at[:, None] == 4 * (at % units) + at // units).astype(jnp.bfloat16)
    half = jnp.where(lax.axis_index("dp") == 0, w_recur[0], w_input[0])
    half = jnp.dot(half, order, preferred_element_type=jnp.float32).astype(jnp.bfloat16)
    weights = lax.all_gather(half, ("col", "dp")).reshape(cols, 2, H, 4 * units)
    weights = pltpu.with_memory_space_constraint(weights, pltpu.HBM)

    kept = keep(weights)

    local_bias = bias[0].reshape(units, 4).T.reshape(1, 4 * units)
    mine = tokens.reshape(steps_count, cols, ROWS, units).transpose(1, 0, 2, 3).astype(jnp.float32)
    sent = jnp.concatenate([mine.reshape(cols, -1), jnp.broadcast_to(local_bias, (cols, 4 * units))], axis=1)
    got = lax.all_to_all(sent, "col", 0, 0, tiled=True)
    x_first = got[:, : steps_count * ROWS * units].reshape(cols, steps_count * ROWS, units).transpose(1, 0, 2)
    x_first = x_first.reshape(chunks, STEPS * ROWS, H).astype(jnp.bfloat16)
    bias_full = got[:, steps_count * ROWS * units :].reshape(1, 4 * H)

    def section(s, carry):
        place, x_sent, hidden, cell, states = carry
        x_got = passed_along(x_sent, "layer", 1)
        product = early(hidden, weights)
        place, hs, x_next, hidden, cell = late(
            place, x_got, x_first, product, hidden, cell, bias_full, kept, weights
        )
        states = lax.dynamic_update_index_in_dim(states, hs, jnp.maximum(s - (layers - 2), 0), 0)
        return place, x_next, hidden, cell, states

    row = jnp.arange(2 * ROWS)[:, None]
    place = jnp.where(row < 4, -level, level) * jnp.ones((1, LANES), jnp.float32)
    zero_x = jnp.zeros((STEPS * ROWS, H), jnp.bfloat16)
    zero_s = jnp.zeros((STEPS * ROWS, H), jnp.float32)
    zero_t = jnp.zeros((chunks + 1, STEPS * ROWS, H), jnp.bfloat16)
    carry = lax.fori_loop(0, stages - 1, section, (place, zero_x, zero_s, zero_s, zero_t))

    moved = lax.all_to_all(carry[4][1:], "layer", 0, 0, tiled=True)[layers - 1]
    _, _, hidden, cell, states = section(stages - 1, carry)
    top = jnp.where(level == layers - 1, states[chunks], moved)
    rows = jnp.concatenate([top.astype(jnp.float32), hidden[:ROWS], cell[:ROWS]], axis=0)
    sent = rows.reshape(4 * ROWS, cols, units).transpose(1, 0, 2)
    got = lax.all_to_all(sent, "col", 0, 0, tiled=True).reshape(cols, 4, ROWS, units).transpose(1, 0, 2, 3)
    got = got.reshape(4, sentences, units)
    return got[:2].astype(jnp.bfloat16), got[2:3].astype(jnp.bfloat16), got[3:]


def solution(mesh):
    in_specs = (
        P(None, "dp", "col"),
        P("layer", None, "col"),
        P("layer", None, "col"),
        P("layer", "col"),
    )
    out_specs = (P("layer", "dp", "col"), P("layer", "dp", "col"), P("layer", "dp", "col"))
    return jax.shard_map(shards, mesh=mesh, in_specs=in_specs, out_specs=out_specs, check_vma=False)
```

```python
import jax
import jax.numpy as jnp
from jax import lax
from jax.experimental import pallas as pl
from jax.experimental.pallas import tpu as pltpu
from jax.sharding import PartitionSpec as P

H = 1024
ROWS = 4
STEPS = 2
LANES = 128
WIDE = 512
BLOCKS = 4 * H // WIDE
KEPT = 11


def passed_along(block, axis, distance):
    devices = range(lax.axis_size(axis))
    route = [(i - distance, i) for i in devices if i - distance in devices]
    return lax.ppermute(block, axis, route)


def segments_swapped(quad, lane):
    gates = []
    for k in range(4):
        out = None
        for j in range(4):
            shift = (32 * (j - k)) % LANES
            moved = quad[j] if shift == 0 else pltpu.roll(quad[j], shift, 1)
            out = moved if out is None else jnp.where(lane >= 32 * j, moved, out)
        gates.append(out)
    return gates


def fetch(weights, close, sems, m, q):
    first = max(4 * q, KEPT) if m == 1 else 4 * q
    pieces = pl.ds(first, 4 * q + 4 - first)
    return pltpu.make_async_copy(weights.at[pieces, m], close.at[m, pieces], sems.at[m, q])


def columns(weights, close, sems, m, q, kept=None):
    here = KEPT if m == 1 else 0
    if here < 4 * q + 4:
        fetch(weights, close, sems, m, q).wait()
    pieces = [kept[p] if p < here else close[m, p] for p in range(4 * q, 4 * q + 4)]
    return jnp.concatenate(pieces, axis=1)


def keep_kernel(weights, kept, sem):
    copy = pltpu.make_async_copy(weights.at[pl.ds(0, KEPT), 1], kept, sem)
    copy.start()
    copy.wait()


def early_kernel(h_was, weights, product_out, close, sems):
    for q in range(BLOCKS):
        fetch(weights, close, sems, 0, q).start()
    h_low = h_was[...].astype(jnp.bfloat16)
    for q in range(BLOCKS):
        part = jnp.dot(h_low, columns(weights, close, sems, 0, q), preferred_element_type=jnp.float32)
        product_out[:, WIDE * q : WIDE * (q + 1)] = part


def late_kernel(place, x_got, x_tokens, product, h_was, c_was, bias, kept, weights, place_out, hs_out, x_out, h_out, c_out, gx, close, sems):
    spot = place[...]
    chunk = jnp.max(spot[0:1, :]).astype(jnp.int32)
    level = jnp.max(spot[4:5, :]).astype(jnp.int32)
    chunks = x_tokens.shape[0]
    active = (chunk >= 0) & (chunk < chunks)
    spot_row = lax.broadcasted_iota(jnp.int32, (2 * ROWS, LANES), 0)
    place_out[...] = jnp.where(spot_row < 4, spot + 1.0, spot)

    @pl.when(active)
    def _():
        for m, done in ((1, KEPT // 4), (0, 0)):
            for q in range(done, BLOCKS):
                fetch(weights, close, sems, m, q).start()
        x = jnp.where(level == 0, x_tokens[chunk].astype(jnp.float32), x_got[...].astype(jnp.float32))
        x_low = x.astype(jnp.bfloat16)
        lane = lax.broadcasted_iota(jnp.int32, (2 * ROWS, LANES), 1)
        row = lax.broadcasted_iota(jnp.int32, (2 * ROWS, H), 0)
        update = (lane >= 64) & (lane < 96)
        scale = jnp.where(update, 1.0, 0.5)
        shift = jnp.where(update, 0.0, 0.5)

        def cells(gates, q, cell):
            quad = []
            for j in range(4):
                lanes = slice(WIDE * q + LANES * j, WIDE * q + LANES * (j + 1))
                z = gates[:, LANES * j : LANES * (j + 1)] * scale + gx[:, lanes]
                quad.append(jnp.tanh(z) * scale + shift)
            g_in, g_forget, g_update, g_out = segments_swapped(quad, lane)
            cell = g_forget * cell + g_in * g_update
            c_out[:, LANES * q : LANES * (q + 1)] = pltpu.roll(cell, ROWS, 0)
            return (g_out * jnp.tanh(cell)).astype(jnp.bfloat16).astype(jnp.float32)

        pieces = []
        for q in range(BLOCKS):
            block = columns(weights, close, sems, 1, q, kept)
            part = jnp.dot(x_low, block, preferred_element_type=jnp.float32)
            for j in range(4):
                lanes = slice(WIDE * q + LANES * j, WIDE * q + LANES * (j + 1))
                gx[:, lanes] = (part[:, LANES * j : LANES * (j + 1)] + bias[:, lanes]) * scale
            here = slice(LANES * q, LANES * (q + 1))
            pieces.append(cells(product[:, WIDE * q : WIDE * (q + 1)], q, c_was[:, here]))
        first = jnp.concatenate(pieces, axis=1)
        h_low = pltpu.roll(first, ROWS, 0).astype(jnp.bfloat16)
        pieces = []
        for q in range(BLOCKS):
            part = jnp.dot(h_low, columns(weights, close, sems, 0, q), preferred_element_type=jnp.float32)
            here = slice(LANES * q, LANES * (q + 1))
            pieces.append(cells(part, q, c_out[:, here]))
        second = jnp.concatenate(pieces, axis=1)
        h_out[...] = pltpu.roll(second, ROWS, 0)
        both = jnp.where(row < ROWS, first, second)
        hs_out[...] = both.astype(jnp.bfloat16)
        x_out[...] = jnp.where(level >= 1, both + x, both).astype(jnp.bfloat16)

    @pl.when(jnp.logical_not(active))
    def _():
        h_out[...] = h_was[...]
        c_out[...] = c_was[...]
        hs_out[...] = x_got[...]
        x_out[...] = x_got[...]


FULL = pl.BlockSpec(memory_space=pltpu.VMEM)
FAR = pl.BlockSpec(memory_space=pltpu.HBM)


def early(h_was, weights):
    return pl.pallas_call(
        early_kernel,
        out_shape=jax.ShapeDtypeStruct((2 * ROWS, 4 * H), jnp.float32),
        in_specs=[FULL, FAR],
        out_specs=FULL,
        scratch_shapes=[pltpu.VMEM((1, H // 32, H, LANES), jnp.bfloat16), pltpu.SemaphoreType.DMA((1, BLOCKS))],
        compiler_params=pltpu.CompilerParams(vmem_limit_bytes=16 * 1024 * 1024),
        cost_estimate=pl.CostEstimate(flops=8_000_000_000, bytes_accessed=8_000_000, transcendentals=0),
    )(h_was, weights)


def keep(weights):
    return pl.pallas_call(
        keep_kernel,
        out_shape=jax.ShapeDtypeStruct((KEPT, H, LANES), jnp.bfloat16),
        in_specs=[FAR],
        out_specs=FULL,
        scratch_shapes=[pltpu.SemaphoreType.DMA],
        compiler_params=pltpu.CompilerParams(vmem_limit_bytes=16 * 1024 * 1024),
    )(weights)


def late(place, x_got, x_tokens, product, h_was, c_was, bias, kept, weights):
    def like(x):
        return jax.ShapeDtypeStruct(x.shape, x.dtype)

    return pl.pallas_call(
        late_kernel,
        out_shape=(like(place), like(x_got), like(x_got), like(h_was), like(c_was)),
        in_specs=[FULL] * 8 + [FAR],
        out_specs=(FULL,) * 5,
        input_output_aliases={0: 0, 4: 3, 5: 4},
        scratch_shapes=[
            pltpu.VMEM((2 * ROWS, 4 * H), jnp.float32),
            pltpu.VMEM((2, H // 32, H, LANES), jnp.bfloat16),
            pltpu.SemaphoreType.DMA((2, BLOCKS)),
        ],
        compiler_params=pltpu.CompilerParams(vmem_limit_bytes=24 * 1024 * 1024),
    )(place, x_got, x_tokens, product, h_was, c_was, bias, kept, weights)


def shards(tokens, w_input, w_recur, bias):
    steps_count, sentences, units = tokens.shape
    layers = lax.axis_size("layer")
    cols = lax.axis_size("col")
    level = lax.axis_index("layer")
    chunks = steps_count // STEPS
    stages = chunks + layers - 1

    at = jnp.arange(4 * units)
    order = (at[:, None] == 4 * (at % units) + at // units).astype(jnp.bfloat16)
    half = jnp.where(lax.axis_index("dp") == 0, w_recur[0], w_input[0])
    half = jnp.dot(half, order, preferred_element_type=jnp.float32).astype(jnp.bfloat16)
    weights = lax.all_gather(half, ("col", "dp")).reshape(cols, 2, H, 4 * units)
    weights = pltpu.with_memory_space_constraint(weights, pltpu.HBM)

    kept = keep(weights)

    local_bias = bias[0].reshape(units, 4).T.reshape(1, 4 * units)
    mine = tokens.reshape(steps_count, cols, ROWS, units).transpose(1, 0, 2, 3).astype(jnp.float32)
    sent = jnp.concatenate([mine.reshape(cols, -1), jnp.broadcast_to(local_bias, (cols, 4 * units))], axis=1)
    got = lax.all_to_all(sent, "col", 0, 0, tiled=True)
    x_first = got[:, : steps_count * ROWS * units].reshape(cols, steps_count * ROWS, units).transpose(1, 0, 2)
    x_first = x_first.reshape(chunks, STEPS * ROWS, H).astype(jnp.bfloat16)
    bias_full = got[:, steps_count * ROWS * units :].reshape(1, 4 * H)

    def section(s, carry):
        place, x_sent, hidden, cell, states = carry
        x_got = passed_along(x_sent, "layer", 1)
        product = early(hidden, weights)
        place, hs, x_next, hidden, cell = late(
            place, x_got, x_first, product, hidden, cell, bias_full, kept, weights
        )
        states = lax.dynamic_update_index_in_dim(states, hs, jnp.maximum(s - (layers - 2), 0), 0)
        return place, x_next, hidden, cell, states

    row = jnp.arange(2 * ROWS)[:, None]
    place = jnp.where(row < 4, -level, level) * jnp.ones((1, LANES), jnp.float32)
    zero_x = jnp.zeros((STEPS * ROWS, H), jnp.bfloat16)
    zero_s = jnp.zeros((STEPS * ROWS, H), jnp.float32)
    zero_t = jnp.zeros((chunks + 1, STEPS * ROWS, H), jnp.bfloat16)
    carry = lax.fori_loop(0, stages - 1, section, (place, zero_x, zero_s, zero_s, zero_t))

    moved = lax.all_to_all(carry[4][1:], "layer", 0, 0, tiled=True)[layers - 1]
    _, _, hidden, cell, states = section(stages - 1, carry)
    top = jnp.where(level == layers - 1, states[chunks], moved)
    rows = jnp.concatenate([top.astype(jnp.float32), hidden[:ROWS], cell[:ROWS]], axis=0)
    sent = rows.reshape(4 * ROWS, cols, units).transpose(1, 0, 2)
    got = lax.all_to_all(sent, "col", 0, 0, tiled=True).reshape(cols, 4, ROWS, units).transpose(1, 0, 2, 3)
    got = got.reshape(4, sentences, units)
    return got[:2].astype(jnp.bfloat16), got[2:3].astype(jnp.bfloat16), got[3:]


def solution(mesh):
    in_specs = (
        P(None, "dp", "col"),
        P("layer", None, "col"),
        P("layer", None, "col"),
        P("layer", "col"),
    )
    out_specs = (P("layer", "dp", "col"), P("layer", "dp", "col"), P("layer", "dp", "col"))
    return jax.shard_map(shards, mesh=mesh, in_specs=in_specs, out_specs=out_specs, check_vma=False)
```

```python
import jax
import jax.numpy as jnp
from jax import lax
from jax.experimental import pallas as pl
from jax.experimental.pallas import tpu as pltpu
from jax.sharding import PartitionSpec as P

H = 1024
ROWS = 4
STEPS = 2
LANES = 128
WIDE = 512
BLOCKS = 4 * H // WIDE
KEPT = 11


def passed_along(block, axis, distance):
    devices = range(lax.axis_size(axis))
    route = [(i - distance, i) for i in devices if i - distance in devices]
    return lax.ppermute(block, axis, route)


def segments_swapped(quad, lane):
    gates = []
    for k in range(4):
        out = None
        for j in range(4):
            shift = (32 * (j - k)) % LANES
            moved = quad[j] if shift == 0 else pltpu.roll(quad[j], shift, 1)
            out = moved if out is None else jnp.where(lane >= 32 * j, moved, out)
        gates.append(out)
    return gates


def fetch(weights, close, sems, m, q):
    first = max(4 * q, KEPT) if m == 1 else 4 * q
    pieces = pl.ds(first, 4 * q + 4 - first)
    return pltpu.make_async_copy(weights.at[pieces, m], close.at[m, pieces], sems.at[m, q])


def columns(weights, close, sems, m, q, kept=None):
    here = KEPT if m == 1 else 0
    if here < 4 * q + 4:
        fetch(weights, close, sems, m, q).wait()
    pieces = [kept[p] if p < here else close[m, p] for p in range(4 * q, 4 * q + 4)]
    return jnp.concatenate(pieces, axis=1)


def keep_kernel(weights, kept, sem):
    copy = pltpu.make_async_copy(weights.at[pl.ds(0, KEPT), 1], kept, sem)
    copy.start()
    copy.wait()


def early_kernel(h_was, weights, product_out, close, sems):
    for q in range(BLOCKS):
        fetch(weights, close, sems, 0, q).start()
    h_low = h_was[...].astype(jnp.bfloat16)
    for q in range(BLOCKS):
        part = jnp.dot(h_low, columns(weights, close, sems, 0, q), preferred_element_type=jnp.float32)
        product_out[:, WIDE * q : WIDE * (q + 1)] = part


def late_kernel(place, x_got, x_tokens, product, h_was, c_was, bias, kept, weights, place_out, hs_out, x_out, h_out, c_out, gx, close, sems):
    spot = place[...]
    chunk = jnp.max(spot[0:1, :]).astype(jnp.int32)
    level = jnp.max(spot[4:5, :]).astype(jnp.int32)
    chunks = x_tokens.shape[0]
    active = (chunk >= 0) & (chunk < chunks)
    spot_row = lax.broadcasted_iota(jnp.int32, (2 * ROWS, LANES), 0)
    place_out[...] = jnp.where(spot_row < 4, spot + 1.0, spot)

    @pl.when(active)
    def _():
        for m, done in ((1, KEPT // 4), (0, 0)):
            for q in range(done, BLOCKS):
                fetch(weights, close, sems, m, q).start()
        x = jnp.where(level == 0, x_tokens[chunk].astype(jnp.float32), x_got[...].astype(jnp.float32))
        x_low = x.astype(jnp.bfloat16)
        lane = lax.broadcasted_iota(jnp.int32, (2 * ROWS, LANES), 1)
        row = lax.broadcasted_iota(jnp.int32, (2 * ROWS, H), 0)
        update = (lane >= 64) & (lane < 96)
        scale = jnp.where(update, 1.0, 0.5)
        shift = jnp.where(update, 0.0, 0.5)

        def cells(gates, q, cell):
            quad = []
            for j in range(4):
                lanes = slice(WIDE * q + LANES * j, WIDE * q + LANES * (j + 1))
                z = gates[:, LANES * j : LANES * (j + 1)] * scale + gx[:, lanes]
                quad.append(jnp.tanh(z) * scale + shift)
            g_in, g_forget, g_update, g_out = segments_swapped(quad, lane)
            cell = g_forget * cell + g_in * g_update
            c_out[:, LANES * q : LANES * (q + 1)] = pltpu.roll(cell, ROWS, 0)
            return (g_out * jnp.tanh(cell)).astype(jnp.bfloat16).astype(jnp.float32)

        pieces = []
        for q in range(BLOCKS):
            block = columns(weights, close, sems, 1, q, kept)
            part = jnp.dot(x_low, block, preferred_element_type=jnp.float32)
            for j in range(4):
                lanes = slice(WIDE * q + LANES * j, WIDE * q + LANES * (j + 1))
                gx[:, lanes] = (part[:, LANES * j : LANES * (j + 1)] + bias[:, lanes]) * scale
            here = slice(LANES * q, LANES * (q + 1))
            pieces.append(cells(product[:, WIDE * q : WIDE * (q + 1)], q, c_was[:, here]))
        first = jnp.concatenate(pieces, axis=1)
        h_low = pltpu.roll(first, ROWS, 0).astype(jnp.bfloat16)
        pieces = []
        for q in range(BLOCKS):
            part = jnp.dot(h_low, columns(weights, close, sems, 0, q), preferred_element_type=jnp.float32)
            here = slice(LANES * q, LANES * (q + 1))
            pieces.append(cells(part, q, c_out[:, here]))
        second = jnp.concatenate(pieces, axis=1)
        h_out[...] = pltpu.roll(second, ROWS, 0)
        both = jnp.where(row < ROWS, first, second)
        hs_out[...] = both.astype(jnp.bfloat16)
        x_out[...] = jnp.where(level >= 1, both + x, both).astype(jnp.bfloat16)

    @pl.when(jnp.logical_not(active))
    def _():
        h_out[...] = h_was[...]
        c_out[...] = c_was[...]
        hs_out[...] = x_got[...]
        x_out[...] = x_got[...]


FULL = pl.BlockSpec(memory_space=pltpu.VMEM)
FAR = pl.BlockSpec(memory_space=pltpu.HBM)


def early(h_was, weights):
    return pl.pallas_call(
        early_kernel,
        out_shape=jax.ShapeDtypeStruct((2 * ROWS, 4 * H), jnp.float32),
        in_specs=[FULL, FAR],
        out_specs=FULL,
        scratch_shapes=[pltpu.VMEM((1, H // 32, H, LANES), jnp.bfloat16), pltpu.SemaphoreType.DMA((1, BLOCKS))],
        compiler_params=pltpu.CompilerParams(vmem_limit_bytes=16 * 1024 * 1024),
        cost_estimate=pl.CostEstimate(flops=8_000_000_000, bytes_accessed=8_000_000, transcendentals=0),
    )(h_was, weights)


def keep(weights):
    return pl.pallas_call(
        keep_kernel,
        out_shape=jax.ShapeDtypeStruct((KEPT, H, LANES), jnp.bfloat16),
        in_specs=[FAR],
        out_specs=FULL,
        scratch_shapes=[pltpu.SemaphoreType.DMA],
        compiler_params=pltpu.CompilerParams(vmem_limit_bytes=16 * 1024 * 1024),
    )(weights)


def late(place, x_got, x_tokens, product, h_was, c_was, bias, kept, weights):
    def like(x):
        return jax.ShapeDtypeStruct(x.shape, x.dtype)

    return pl.pallas_call(
        late_kernel,
        out_shape=(like(place), like(x_got), like(x_got), like(h_was), like(c_was)),
        in_specs=[FULL] * 8 + [FAR],
        out_specs=(FULL,) * 5,
        input_output_aliases={0: 0, 4: 3, 5: 4},
        scratch_shapes=[
            pltpu.VMEM((2 * ROWS, 4 * H), jnp.float32),
            pltpu.VMEM((2, H // 32, H, LANES), jnp.bfloat16),
            pltpu.SemaphoreType.DMA((2, BLOCKS)),
        ],
        compiler_params=pltpu.CompilerParams(vmem_limit_bytes=24 * 1024 * 1024),
    )(place, x_got, x_tokens, product, h_was, c_was, bias, kept, weights)


def shards(tokens, w_input, w_recur, bias):
    steps_count, sentences, units = tokens.shape
    layers = lax.axis_size("layer")
    cols = lax.axis_size("col")
    level = lax.axis_index("layer")
    chunks = steps_count // STEPS
    stages = chunks + layers - 1

    at = jnp.arange(4 * units)
    order = (at[:, None] == 4 * (at % units) + at // units).astype(jnp.bfloat16)
    half = jnp.where(lax.axis_index("dp") == 0, w_recur[0], w_input[0])
    half = jnp.dot(half, order, preferred_element_type=jnp.float32).astype(jnp.bfloat16)
    weights = lax.all_gather(half, ("col", "dp")).reshape(cols, 2, H, 4 * units)
    weights = pltpu.with_memory_space_constraint(weights, pltpu.HBM)

    kept = keep(weights)

    local_bias = bias[0].reshape(units, 4).T.reshape(1, 4 * units)
    mine = tokens.reshape(steps_count, cols, ROWS, units).transpose(1, 0, 2, 3)
    high = lax.reduce_precision(local_bias, 8, 7)
    middle = lax.reduce_precision(local_bias - high, 8, 7)
    parts = jnp.concatenate([high, middle, local_bias - high - middle], axis=1).astype(jnp.bfloat16)
    sent = jnp.concatenate([mine.reshape(cols, -1), jnp.broadcast_to(parts, (cols, 12 * units))], axis=1)
    got = lax.all_to_all(sent, "col", 0, 0, tiled=True)
    x_first = got[:, : steps_count * ROWS * units].reshape(cols, steps_count * ROWS, units).transpose(1, 0, 2)
    x_first = x_first.reshape(chunks, STEPS * ROWS, H)
    parts = got[:, steps_count * ROWS * units :].astype(jnp.float32).reshape(cols, 3, 4 * units)
    bias_full = (parts[:, 0] + parts[:, 1] + parts[:, 2]).reshape(1, 4 * H)

    def section(s, carry):
        place, x_sent, hidden, cell, states = carry
        x_got = passed_along(x_sent, "layer", 1)
        product = early(hidden, weights)
        place, hs, x_next, hidden, cell = late(
            place, x_got, x_first, product, hidden, cell, bias_full, kept, weights
        )
        states = lax.dynamic_update_index_in_dim(states, hs, jnp.maximum(s - (layers - 2), 0), 0)
        return place, x_next, hidden, cell, states

    row = jnp.arange(2 * ROWS)[:, None]
    place = jnp.where(row < 4, -level, level) * jnp.ones((1, LANES), jnp.float32)
    zero_x = jnp.zeros((STEPS * ROWS, H), jnp.bfloat16)
    zero_s = jnp.zeros((STEPS * ROWS, H), jnp.float32)
    zero_t = jnp.zeros((chunks + 1, STEPS * ROWS, H), jnp.bfloat16)
    carry = lax.fori_loop(0, stages - 1, section, (place, zero_x, zero_s, zero_s, zero_t))

    moved = lax.all_to_all(carry[4][1:], "layer", 0, 0, tiled=True)[layers - 1]
    _, _, hidden, cell, states = section(stages - 1, carry)
    top = jnp.where(level == layers - 1, states[chunks], moved)
    rows = jnp.concatenate([top.astype(jnp.float32), hidden[:ROWS], cell[:ROWS]], axis=0)
    sent = rows.reshape(4 * ROWS, cols, units).transpose(1, 0, 2).reshape(cols, 4, ROWS * units)
    got = lax.all_to_all(sent, "col", 0, 0, tiled=True).reshape(cols, 4, ROWS, units).transpose(1, 0, 2, 3)
    got = got.reshape(4, sentences, units)
    return got[:2].astype(jnp.bfloat16), got[2:3].astype(jnp.bfloat16), got[3:]


def solution(mesh):
    in_specs = (
        P(None, "dp", "col"),
        P("layer", None, "col"),
        P("layer", None, "col"),
        P("layer", "col"),
    )
    out_specs = (P("layer", "dp", "col"), P("layer", "dp", "col"), P("layer", "dp", "col"))
    return jax.shard_map(shards, mesh=mesh, in_specs=in_specs, out_specs=out_specs, check_vma=False)
```
